32 devices in a mesh: col: 8 (over y, x, core), row: 4 (over z).
Axes of the slice: x: 2, y: 2, z: 4, core: 2. Of those that a mesh axis runs over, the one named last changes fastest.
Arguments:
- trace_start: float32 [32, 32768], P(None, ('col', 'row')), may hold values from -6 to 6
- surface_load: float32 [32, 32768], P(None, ('col', 'row')), may hold values from -6 to 6
- panel_tiles: bfloat16 [704, 512, 512], P(('col', 'row')), may hold values from -0.03125 to 0.03125
- tile_list: int32 [704], P(('col', 'row')), may hold values from -1 to 4095, as said below
- surf_map: int32 [8], replicated, may hold values from 0 to 7, as said below
- coef_index: int32 [2, 4, 16384], P(None, None, 'row'), may hold values from 0 to 15
- coef_table: float32 [16], replicated, may hold values from 0.2 to 2
- vol_source: float32 [2, 4, 16384], P(None, None, 'row'), may hold values from -6 to 6
Outputs:
- traces: float32 [32, 32768], P(None, ('col', 'row'))
- response: float32 [32, 32768], P(None, ('col', 'row'))
The draws below stay inside these ranges and needn't reach their ends.
Inputs may be any that keep to these rules, and one draw needn't show every extreme that they name: `tile_list`: each device has 22 slots, ordered by col index, then row index, then slot. A value i * 64 + j names the tile of rows i * 512 to (i + 1) * 512 - 1 and columns j * 512 to (j + 1) * 512 - 1 of the boundary matrix, with j <= i and j < 8; each such tile is named exactly once. A device of col index c and row index r names only tiles whose rows lie in shards of row index r (i * 512 // 1024 leaves remainder r modulo 4), and none if c >= 6; its named tiles fill its first slots and the rest hold -1. Some device names 22 tiles. surf_map[r * 2 + q] leaves remainder r modulo 4; each volume tile lies under exactly one surface tile.
All inputs are finite; a program needn't handle non-finite values.
Results may differ from the reference program's by a relative error of at most 0.0041.
Values may be sent and summed in bfloat16 or wider, within the bound.
A program may use at most 128 MiB of HBM per device.

```python
import math
import jax
import jax.numpy as jnp
import numpy as np
from jax import lax

RHS = 32
NODES = 4096
TILE = 512
LAYERS = 4
ITERS = 2
SWEEPS = 4
COEFS = 16
VOL_COLS = 2
DENSE_COLS = 6
SURFACE = 32768
SHARD = 1024
WIN_TILES = 8
SIDE = 64
SLOTS_DEV = 22
SLOTS = 704
SURF_TILES = 8
LINE = 16384
N_COL = 8
N_ROW = 4


def draw_tile_list(key, part):
    per_shard = SHARD // TILE
    slot_table = jnp.full((N_COL, N_ROW, SLOTS_DEV), -1, jnp.int32)
    for row_block in range(N_ROW):
        tile_names = []
        for tile_row in range(SIDE):
            if tile_row // per_shard % N_ROW == row_block:
                for tile_col in range(min(tile_row + 1, WIN_TILES)):
                    tile_names.append(tile_row * SIDE + tile_col)
        name_table = jnp.asarray(np.array(tile_names, dtype=np.int32))
        name_count = len(tile_names)
        key_order = jax.random.fold_in(key, 2 * row_block + 11)
        key_columns = jax.random.fold_in(key, 2 * row_block + 12)
        tile_order = jax.random.permutation(key_order, name_count)
        column_order = jax.random.permutation(key_columns, DENSE_COLS)
        placing = np.arange(name_count)
        slot_table = slot_table.at[column_order[placing % DENSE_COLS], row_block, placing // DENSE_COLS].set(name_table[tile_order])
    return slot_table.reshape(-1)


def draw_surf_map(key, part):
    pieces = []
    for row_block in range(N_ROW):
        order = jax.random.permutation(jax.random.fold_in(key, 101 + row_block), VOL_COLS).astype(jnp.int32)
        pieces.append(order * N_ROW + row_block)
    return jnp.concatenate(pieces)


def plant(values, rng, smallest, largest):
    spot = [jax.random.randint(jax.random.fold_in(rng, axis), (), 0, length) for axis, length in enumerate(values.shape)]
    longest = values.shape.index(max(values.shape))
    neighbour = spot[:longest] + [(spot[longest] + 1) % values.shape[longest]] + spot[longest + 1:]
    return values.at[tuple(spot)].set(smallest).at[tuple(neighbour)].set(largest)


def level_of(own_key, extent, split, low, high):
    def one(dim, parts):
        steps = jax.random.uniform(jax.random.fold_in(jax.random.fold_in(own_key, 6), dim), (parts,), jnp.float32, low / len(split), high / len(split))
        return jnp.repeat(jnp.exp(steps), extent[dim] // parts).reshape((-1,) + (1,) * (len(extent) - dim - 1))

    gain = one(*split[0])
    for cut in split[1:]:
        gain = gain * one(*cut)
    return gain


def scatter_about(own_key, extent, scale, bound, shards=(), held_as=jnp.bfloat16):
    factor_of = level_of(own_key, extent, shards, -0.22, 0.18) if shards else 1.0
    values = jax.random.normal(own_key, extent, jnp.float32) * scale * factor_of
    return jnp.minimum(jnp.maximum(values, -bound), bound).astype(held_as)


def setup_inputs(seed: int = 0) -> dict:
    key_list = jax.random.split(jax.random.key(seed), 9)
    trace_start = scatter_about(key_list[0], (RHS, SURFACE), 1.0, 6.0, ((1, 32),), jnp.float32)
    surface_load = scatter_about(key_list[1], (RHS, SURFACE), 1.0, 6.0, ((1, 32),), jnp.float32)
    panel_tiles = scatter_about(key_list[2], (SLOTS, TILE, TILE), SURFACE ** -0.5, 0.03125, ((0, 32),))
    tile_list = draw_tile_list(jax.random.fold_in(key_list[8], 71), 0)
    surf_map = draw_surf_map(jax.random.fold_in(key_list[8], 71), 0)
    coef_index = plant(jax.random.randint(key_list[5], (VOL_COLS, LAYERS, LINE), 0, COEFS), jax.random.fold_in(key_list[5], 1), 0, COEFS - 1).astype(jnp.int32)
    coef_table = jnp.clip(jnp.exp(jax.random.uniform(key_list[6], (COEFS,), jnp.float32, math.log(0.2), math.log(2.0))), 0.2, 2.0)
    vol_source = scatter_about(key_list[7], (VOL_COLS, LAYERS, LINE), 1.0, 6.0, ((2, 4),), jnp.float32)
    return {"trace_start": trace_start, "surface_load": surface_load, "panel_tiles": panel_tiles, "tile_list": tile_list, "surf_map": surf_map, "coef_index": coef_index, "coef_table": coef_table, "vol_source": vol_source}


COUPLING_STEP = 0.3
JACOBI_WEIGHT = 0.8
CELL_MASS = 0.05


def lookup_coefs(indices, coef_values):
    levels = jnp.arange(coef_values.shape[0], dtype=jnp.int32)
    return jnp.sum(jnp.where(indices[..., None] == levels, coef_values, 0.0), axis=-1)


def relax_line(padded_values, coefs_pad, source, top_trace):
    centre_coef = coefs_pad[:, 1:-1]
    left_weight = 0.5 * (centre_coef + coefs_pad[:, :-2])
    right_weight = 0.5 * (centre_coef + coefs_pad[:, 2:])
    layer_weight = 0.5 * (centre_coef[:-1] + centre_coef[1:])
    upper_weight = jnp.concatenate([centre_coef[:1], layer_weight], 0)
    lower_weight = jnp.concatenate([layer_weight, jnp.zeros_like(centre_coef[:1])], 0)
    centre = padded_values[:, :, 1:-1]
    upper_values = jnp.concatenate([top_trace[:, None, :], centre[:, :-1]], 1)
    lower_values = jnp.concatenate([centre[:, 1:], jnp.zeros_like(centre[:, :1])], 1)
    gathered = (left_weight * padded_values[:, :, :-2] + right_weight * padded_values[:, :, 2:]
                + upper_weight * upper_values + lower_weight * lower_values + source)
    diagonal = left_weight + right_weight + upper_weight + lower_weight + CELL_MASS
    return (1.0 - JACOBI_WEIGHT) * centre + JACOBI_WEIGHT * gathered / diagonal


def add_block(partial_value, block_sum, block_start):
    current = lax.dynamic_slice_in_dim(partial_value, block_start, TILE, 1)
    return lax.dynamic_update_slice_in_dim(partial_value, current + block_sum, block_start, 1)


def to_bands(values):
    return values.reshape(RHS, N_COL, N_ROW, SHARD).transpose(0, 2, 1, 3).reshape(RHS, SURFACE)


def from_bands(values):
    return values.reshape(RHS, N_ROW, N_COL, SHARD).transpose(0, 2, 1, 3).reshape(RHS, SURFACE)


def panel_product(whole_traces, panel_tiles, tile_list):
    def advance(partial_value, item):
        panel_block, tile_ident = item

        def accumulate(current):
            row_start = ((tile_ident // SIDE) * TILE).astype(jnp.int32)
            col_start = ((tile_ident % SIDE) * TILE).astype(jnp.int32)
            row_part = lax.dynamic_slice_in_dim(whole_traces, row_start, TILE, 1)
            col_part = lax.dynamic_slice_in_dim(whole_traces, col_start, TILE, 1)
            into_rows = lax.dot_general(col_part, panel_block, (((1,), (1,)), ((), ())),
                                        preferred_element_type=jnp.float32)
            into_cols = jnp.dot(row_part, panel_block, preferred_element_type=jnp.float32)
            current = add_block(current, into_rows, row_start)
            return add_block(current, into_cols, col_start)

        partial_value = lax.cond(tile_ident >= 0, accumulate, lambda current: current, partial_value)
        return partial_value, None

    start_sum = jnp.zeros((RHS, SURFACE), jnp.float32)
    result, _ = lax.scan(advance, start_sum, (panel_tiles, tile_list))
    return result


def reference(trace_start, surface_load, panel_tiles, tile_list, surf_map, coef_index, coef_table, vol_source):
    coef_lines = lookup_coefs(coef_index, coef_table)
    coef_padded = jnp.pad(coef_lines, ((0, 0), (0, 0), (1, 1)))
    inverse_map = jnp.zeros((SURF_TILES,), jnp.int32).at[surf_map].set(jnp.arange(SURF_TILES, dtype=jnp.int32))
    volume_states = [jnp.zeros((RHS, LAYERS, LINE), jnp.float32) for line_index in range(VOL_COLS)]
    traces = trace_start
    response = trace_start
    for iteration in range(ITERS):
        whole_traces = traces.astype(jnp.bfloat16)
        products = panel_product(whole_traces, panel_tiles, tile_list)
        surface_tiles = to_bands(whole_traces.astype(jnp.float32)).reshape(RHS, SURF_TILES, NODES)
        line_traces = surface_tiles[:, inverse_map].reshape(RHS, VOL_COLS, LINE)
        fluxes = []
        for line_index in range(VOL_COLS):
            top_trace = line_traces[:, line_index]
            volume_state = volume_states[line_index]
            for sweep_index in range(SWEEPS):
                padded_state = jnp.pad(volume_state, ((0, 0), (0, 0), (1, 1)))
                volume_state = relax_line(padded_state, coef_padded[line_index], vol_source[line_index], top_trace)
            volume_states[line_index] = volume_state
            fluxes.append(coef_lines[line_index, 0] * (top_trace - volume_state[:, 0]))
        flux_lines = jnp.stack(fluxes, 1).reshape(RHS, SURF_TILES, NODES)
        flux_surface = from_bands(flux_lines[:, surf_map].reshape(RHS, SURFACE))
        response = products + flux_surface
        traces = traces + COUPLING_STEP * (surface_load - traces - response)
    return traces, response
```

```python
import functools

import jax
import jax.numpy as jnp
from jax import lax
from jax.experimental import pallas as pl
from jax.experimental.pallas import tpu as pltpu
from jax.sharding import PartitionSpec as P

ITERS = 2
SWEEPS = 4

COUPLING_STEP = 0.3
JACOBI_WEIGHT = 0.8
CELL_MASS = 0.05

LANES = 128
SUB = 8
F32 = jnp.float32
BF16 = jnp.bfloat16


def kernel(
    cfg,
    row_tile_ref,
    col_tile_ref,
    slot_ref,
    surf_ref,
    table_ref,
    start_ref,
    load_ref,
    index_ref,
    source_ref,
    panel_hbm,
    traces_ref,
    response_ref,
    panel,
    own,
    band,
    window,
    edge_left,
    edge_right,
    halo_index,
    halo_source,
    product,
    window_part,
    window_recv,
    row_part,
    row_recv,
    coef_ext,
    source_ext,
    weights,
    state,
    top,
    panel_sem,
    band_send,
    band_recv,
    win_send,
    win_recv,
    edge_send,
    edge_recv,
    halo_send,
    halo_recv,
    part_send,
    part_recv,
    row_send,
    row_rsem,
    band_now,
    window_now,
    edge_now,
):
    cols, rows, lines, per_shard, tile, slots, nodes, layers, rhs, levels = cfg
    dense = cols - lines
    group = cols // lines
    shard = per_shard * tile
    win_tiles = rows * per_shard
    c = lax.axis_index("col")
    r = lax.axis_index("row")
    vol = jnp.maximum(c - dense, 0)
    row_up = jnp.minimum(r + 1, rows - 1)
    row_down = jnp.maximum(r - 1, 0)
    is_volume = c >= dense
    is_dense = c < dense
    first_of_tile = (lax.rem(c, group) == 0) & (r > 0)
    last_of_tile = (lax.rem(c, group) == group - 1) & (r < rows - 1)
    has_left = r > 0
    has_right = r < rows - 1

    def copy(src, dst, send, recv, to_col, to_row):
        return pltpu.make_async_remote_copy(
            src_ref=src,
            dst_ref=dst,
            send_sem=send,
            recv_sem=recv,
            device_id=(to_col, to_row),
            device_id_type=pl.DeviceIdType.MESH,
        )

    def col_peer(k):
        return lax.rem(c + k, cols)

    def row_peer(k):
        return lax.rem(r + k, rows)

    def panel_copy(s):
        return pltpu.make_async_copy(panel_hbm.at[s], panel.at[s], panel_sem.at[s])

    @pl.when(is_dense)
    def _():
        def start(s, _):
            panel_copy(s).start()
            return 0

        lax.fori_loop(0, slots, start, 0)

    barrier = pltpu.get_barrier_semaphore()

    def greet(to_col, to_row):
        pl.semaphore_signal(
            barrier, inc=1, device_id=(to_col, to_row), device_id_type=pl.DeviceIdType.MESH
        )

    for k in range(1, cols):
        greet(col_peer(k), r)
    for k in range(1, rows):
        greet(c, row_peer(k))

    @pl.when(last_of_tile)
    def _():
        for v in range(lines):
            greet(dense + v, row_up)

    @pl.when(first_of_tile)
    def _():
        for v in range(lines):
            greet(dense + v, row_down)

    @pl.when(is_volume & has_left)
    def _():
        for q in range(lines):
            greet(q * group + group - 1, row_down)

    @pl.when(is_volume & has_right)
    def _():
        for q in range(lines):
            greet(q * group, row_up)

    def count(flag):
        return jnp.where(flag, lines, 0)

    expected = (
        cols
        - 1
        + rows
        - 1
        + count(last_of_tile)
        + count(first_of_tile)
        + count(is_volume & has_left)
        + count(is_volume & has_right)
    )
    traces_ref[...] = start_ref[...]
    product[slots] = jnp.zeros((rhs, tile), F32)
    pl.semaphore_wait(barrier, expected)

    def halo_copy(kind, side, arrival=False):
        ref = (index_ref, source_ref)[kind]
        dst = (halo_index, halo_source)[kind]
        at = nodes - LANES if side == 0 else 0
        to = row_up if (side == 0) != arrival else row_down
        return copy(
            ref.at[:, :, pl.ds(at, LANES)],
            dst.at[side],
            halo_send.at[kind, side],
            halo_recv.at[kind, side],
            c,
            to,
        )

    sides = ((0, has_right, has_left), (1, has_left, has_right))
    for side, sends, _ in sides:

        @pl.when(is_volume & sends)
        def _():
            for kind in range(2):
                halo_copy(kind, side).start()

    def band_copy(it, k):
        to = col_peer(k)
        return copy(own.at[it], band.at[it, c], band_send.at[it, k], band_recv.at[it, c], to, r)

    def band_arrival(it, src):
        return copy(own.at[it], band.at[it, src], band_send.at[it, 0], band_recv.at[it, src], src, r)

    def edge_copy(it, side, v):
        q = lax.div(c, group)
        if side == 0:
            src = own.at[it, per_shard - 1, :, pl.ds(tile - LANES, LANES)]
            dst, to = edge_left, row_up
        else:
            src = own.at[it, 0, :, pl.ds(0, LANES)]
            dst, to = edge_right, row_down
        return copy(
            src,
            dst.at[it, q],
            edge_send.at[it, side, v],
            edge_recv.at[it, side, q],
            dense + v,
            to,
        )

    def edge_arrival(it, side, q):
        dst = (edge_left, edge_right)[side]
        src = own.at[it, 0, :, pl.ds(0, LANES)]
        if side == 0:
            from_col, from_row = q * group + group - 1, row_down
        else:
            from_col, from_row = q * group, row_up
        return copy(
            src,
            dst.at[it, q],
            edge_send.at[it, side, 0],
            edge_recv.at[it, side, q],
            from_col,
            from_row,
        )

    def window_copy(it, k):
        to = row_peer(k)
        return copy(band.at[it, 0], window.at[it, r], win_send.at[it, k], win_recv.at[it, r], c, to)

    def window_arrival(it, k):
        src = row_peer(k)
        return copy(
            band.at[it, 0], window.at[it, src], win_send.at[it, k], win_recv.at[it, src], c, src
        )

    def part_copy(it, k):
        to = row_peer(k)
        return copy(
            window_part.at[it, to],
            window_recv.at[it, r],
            part_send.at[it, k],
            part_recv.at[it, r],
            c,
            to,
        )

    def part_arrival(it, k):
        src = row_peer(k)
        return copy(
            window_part.at[it, src],
            window_recv.at[it, src],
            part_send.at[it, k],
            part_recv.at[it, src],
            c,
            src,
        )

    def row_copy(it, to):
        return copy(
            row_part.at[it, to], row_recv.at[it, c], row_send.at[it, to], row_rsem.at[it, c], to, r
        )

    def row_arrival(it, src):
        return copy(
            row_part.at[it, src],
            row_recv.at[it, src],
            row_send.at[it, src],
            row_rsem.at[it, src],
            src,
            r,
        )

    def prepare_volume():
        line = lax.div(surf_ref[r * lines + vol], rows)
        padded = nodes + 4 * LANES
        for side, _, receives in sides:

            @pl.when(receives)
            def _():
                for kind in range(2):
                    halo_copy(kind, side, True).wait_recv()

            @pl.when(jnp.logical_not(receives))
            def _():
                halo_index[side] = jnp.zeros((lines, layers, LANES), jnp.int32)
                halo_source[side] = jnp.zeros((lines, layers, LANES), F32)

        def lookup(indices):
            values = jnp.zeros(indices.shape, F32)
            for level in range(levels):
                values = jnp.where(indices == level, table_ref[level], values)
            return values

        zeros = jnp.zeros((layers, LANES), F32)
        left_on = jnp.where(has_left, 1.0, 0.0)
        right_on = jnp.where(has_right, 1.0, 0.0)
        right_at = 2 * LANES + nodes
        coef_ext[:, 0:LANES] = zeros
        coef_ext[:, LANES : 2 * LANES] = lookup(halo_index[0, line]) * left_on
        coef_ext[:, 2 * LANES : right_at] = lookup(index_ref[line])
        coef_ext[:, right_at : right_at + LANES] = lookup(halo_index[1, line]) * right_on
        coef_ext[:, right_at + LANES :] = zeros
        source_ext[:, 0:LANES] = zeros
        source_ext[:, LANES : 2 * LANES] = halo_source[0, line]
        source_ext[:, 2 * LANES : right_at] = source_ref[line]
        source_ext[:, right_at : right_at + LANES] = halo_source[1, line]
        source_ext[:, right_at + LANES :] = zeros
        lane = lax.broadcasted_iota(jnp.int32, (1, padded), 1)
        low = jnp.where(has_left, LANES, 2 * LANES)
        high = jnp.where(has_right, right_at + LANES, right_at)
        inside = (lane >= low) & (lane < high)
        for layer in range(layers):
            k = coef_ext[layer : layer + 1, :]
            left = 0.5 * (k + pltpu.roll(k, 1, 1))
            right = 0.5 * (k + pltpu.roll(k, padded - 1, 1))
            up = 0.5 * (k + coef_ext[layer - 1 : layer, :]) if layer else k
            diagonal = left + right + up + CELL_MASS
            parts = [left, right, up]
            if layer < layers - 1:
                down = 0.5 * (k + coef_ext[layer + 1 : layer + 2, :])
                diagonal = diagonal + down
                parts.append(down)
            else:
                parts.append(None)
            parts.append(source_ext[layer : layer + 1, :])
            scale = jnp.where(inside, JACOBI_WEIGHT / diagonal, 0.0)
            for kind, part in enumerate(parts):
                if part is not None:
                    weights[kind, layer] = jnp.broadcast_to(part * scale, (SUB, padded))
        top[:, 0:LANES] = jnp.zeros((rhs, LANES), F32)
        top[:, right_at + LANES :] = jnp.zeros((rhs, LANES), F32)
        for layer in range(layers):
            state[0, layer] = jnp.zeros((rhs, padded), F32)
            state[1, layer, :, 0:LANES] = jnp.zeros((rhs, LANES), F32)
            state[1, layer, :, right_at + LANES :] = jnp.zeros((rhs, LANES), F32)

    def relax(now, at, width):
        span = width + 2 * LANES
        begin = pl.multiple_of(at - LANES, LANES)
        at = pl.multiple_of(at, LANES)
        for layer in range(layers):
            factors = [
                None if kind == 3 and layer == layers - 1 else weights[kind, layer, :, pl.ds(at, width)]
                for kind in range(5)
            ]
            for g in range(rhs // SUB):
                lines_at = pl.ds(g * SUB, SUB)
                around = state[now, layer, lines_at, pl.ds(begin, span)]
                centre = around[:, LANES : LANES + width]
                before = pltpu.roll(around, 1, 1)[:, LANES : LANES + width]
                after = pltpu.roll(around, span - 1, 1)[:, LANES : LANES + width]
                if layer:
                    above = state[now, layer - 1, lines_at, pl.ds(at, width)]
                else:
                    above = top[lines_at, pl.ds(at, width)]
                value = (1.0 - JACOBI_WEIGHT) * centre + factors[4]
                value = value + factors[0] * before + factors[1] * after + factors[2] * above
                if layer < layers - 1:
                    value = value + factors[3] * state[now, layer + 1, lines_at, pl.ds(at, width)]
                state[1 - now, layer, lines_at, pl.ds(at, width)] = value

    def volume(it):
        q = vol
        right_at = 2 * LANES + nodes
        for m in range(group):
            src = q * group + m

            @pl.when(src != c)
            def _():
                band_arrival(it, src).wait_recv()

            for p in range(per_shard):
                at = 2 * LANES + m * shard + p * tile
                top[:, at : at + tile] = band[it, src, p].astype(F32)
        line = lax.div(surf_ref[r * lines + q], rows)
        for side, _, receives in sides:
            dst = (edge_left, edge_right)[side]
            at = LANES if side == 0 else right_at
            base = row_down if side == 0 else row_up
            place = 0
            for z in range(lines):
                place = jnp.where(surf_ref[base * lines + z] == line * rows + base, z, place)

            @pl.when(receives)
            def _():
                for z in range(lines):
                    edge_arrival(it, side, z).wait_recv()
                for z in range(lines):
                    edge_now[z] = dst[it, z]
                top[:, at : at + LANES] = edge_now[place].astype(F32)

            @pl.when(jnp.logical_not(receives))
            def _():
                top[:, at : at + LANES] = jnp.zeros((rhs, LANES), F32)

        def sweep(i, _):
            now = lax.rem(i, 2)
            relax(now, LANES, LANES)
            relax(now, right_at, LANES)

            def chunk(j, _):
                relax(now, 2 * LANES + j * tile, tile)
                return 0

            lax.fori_loop(0, nodes // tile, chunk, 0)
            return 0

        lax.fori_loop(0, SWEEPS, sweep, 0)
        done = SWEEPS % 2
        for m in range(group):
            to = q * group + m
            for p in range(per_shard):
                at = 2 * LANES + m * shard + p * tile
                k = index_coef(at)
                flux = k * (top[:, at : at + tile] - state[done, 0, :, at : at + tile])
                row_part[it, to, p] = flux.astype(BF16)

            @pl.when(to != c)
            def _():
                row_copy(it, to).start()

    def index_coef(at):
        return coef_ext[0:1, at : at + tile]

    def total_of(tiles_of):
        value = product[tiles_of[0]]
        for t in tiles_of[1:]:
            value = value + product[t]
        return value

    def dense_part(it):
        @pl.when(c != 0)
        def _():
            band_arrival(it, 0).wait_recv()

        for k in range(1, rows):
            window_copy(it, k).start()
        window[it, r] = band[it, 0]
        for src in range(1, cols):

            @pl.when(c != src)
            def _():
                band_arrival(it, src).wait_recv()

        for src in range(cols):
            band_now[src] = band[it, src]

        def into_cols(s, _):
            @pl.when(it == 0)
            def _():
                panel_copy(s).wait()

            row_tile = row_tile_ref[s]
            traces = band_now[lax.div(row_tile, per_shard), lax.rem(row_tile, per_shard)]
            product[s] = jnp.dot(traces, panel[s], preferred_element_type=F32)
            return 0

        lax.fori_loop(0, slots, into_cols, 0)
        band_tiles = cols * per_shard

        def sum_window(j, _):
            value = total_of([slot_ref[b * win_tiles + j] for b in range(band_tiles)])
            window_part[it, lax.div(j, per_shard), lax.rem(j, per_shard)] = value.astype(BF16)
            return 0

        lax.fori_loop(0, win_tiles, sum_window, 0)
        for k in range(1, rows):
            part_copy(it, k).start()
        for k in range(1, rows):
            window_arrival(it, k).wait_recv()

        for src in range(rows):
            window_now[src] = window[it, src]

        def into_rows(s, _):
            col_tile = col_tile_ref[s]
            traces = window_now[lax.div(col_tile, per_shard), lax.rem(col_tile, per_shard)]
            product[s] = lax.dot_general(
                traces, panel[s], (((1,), (1,)), ((), ())), preferred_element_type=F32
            )
            return 0

        lax.fori_loop(0, slots, into_rows, 0)

        def sum_rows(b, _):
            value = total_of([slot_ref[b * win_tiles + j] for j in range(win_tiles)])
            row_part[it, lax.div(b, per_shard), lax.rem(b, per_shard)] = value.astype(BF16)
            return 0

        lax.fori_loop(per_shard, band_tiles, sum_rows, 0)
        for to in range(1, cols):

            @pl.when(c != to)
            def _():
                row_copy(it, to).start()

        for k in range(1, rows):
            part_arrival(it, k).wait_recv()
        for p in range(per_shard):
            value = total_of([slot_ref[p * win_tiles + j] for j in range(win_tiles)])
            value = value + window_part[it, r, p].astype(F32)
            for k in range(1, rows):
                value = value + window_recv[it, row_peer(k), p].astype(F32)
            row_part[it, 0, p] = value.astype(BF16)

        @pl.when(c != 0)
        def _():
            row_copy(it, 0).start()

    def iteration(it, _):
        for p in range(per_shard):
            rounded = traces_ref[:, p * tile : (p + 1) * tile].astype(BF16)
            own[it, p] = rounded
            band[it, c, p] = rounded
        for k in range(1, cols):
            band_copy(it, k).start()
        for side, flag in ((0, last_of_tile), (1, first_of_tile)):

            @pl.when(flag)
            def _():
                for v in range(lines):
                    edge_copy(it, side, v).start()

        @pl.when(is_volume)
        def _():
            @pl.when(it == 0)
            def _():
                prepare_volume()

            volume(it)
            for k in range(cols):

                @pl.when((k != c) & (k // group != c - dense))
                def _():
                    band_arrival(it, k).wait_recv()

        @pl.when(is_dense)
        def _():
            dense_part(it)

        owner = dense + lax.div(c, group)
        for src in range(cols):

            @pl.when((src != c) & ((src < dense) | (src == owner)))
            def _():
                row_arrival(it, src).wait_recv()

        def own_part(p):
            return row_part[it, c, p].astype(F32)

        for p in range(per_shard):
            at = slice(p * tile, (p + 1) * tile)
            response_ref[:, at] = jnp.zeros((rhs, tile), F32)
            for src in range(dense):

                @pl.when(src != c)
                def _():
                    response_ref[:, at] += row_recv[it, src, p].astype(F32)

            @pl.when(owner != c)
            def _():
                response_ref[:, at] += row_recv[it, owner, p].astype(F32)

            @pl.when(is_dense | (owner == c))
            def _():
                response_ref[:, at] += own_part(p)

            t = traces_ref[:, at]
            traces_ref[:, at] = t + COUPLING_STEP * (load_ref[:, at] - t - response_ref[:, at])
        return 0

    lax.fori_loop(0, ITERS, iteration, 0)

    def drain(it, _):
        for k in range(1, cols):
            band_copy(it, k).wait_send()
        for side, flag in ((0, last_of_tile), (1, first_of_tile)):

            @pl.when(flag)
            def _():
                for v in range(lines):
                    edge_copy(it, side, v).wait_send()

        @pl.when(is_dense)
        def _():
            for k in range(1, rows):
                window_copy(it, k).wait_send()
                part_copy(it, k).wait_send()
            for to in range(cols):

                @pl.when(c != to)
                def _():
                    row_copy(it, to).wait_send()

        @pl.when(is_volume)
        def _():
            for m in range(group):
                to = vol * group + m

                @pl.when(to != c)
                def _():
                    row_copy(it, to).wait_send()

        return 0

    lax.fori_loop(0, ITERS, drain, 0)
    for side, sends, _ in sides:

        @pl.when(is_volume & sends)
        def _():
            for kind in range(2):
                halo_copy(kind, side).wait_send()


def local(
    trace_start, surface_load, panel_tiles, tile_list, surf_map, coef_index, coef_table, vol_source
):
    cols = lax.axis_size("col")
    rows = lax.axis_size("row")
    row_index = lax.axis_index("row")
    lines, layers, nodes = coef_index.shape
    slots, tile, _ = panel_tiles.shape
    rhs, shard = trace_start.shape
    per_shard = shard // tile
    levels = coef_table.shape[0]
    side = cols * rows * per_shard
    band_tiles = cols * per_shard
    win_tiles = rows * per_shard
    safe = jnp.maximum(tile_list, 0)
    row_tile = safe // side
    col_tile = safe % side
    band_tile = row_tile // per_shard // rows * per_shard + row_tile % per_shard
    b = jnp.arange(band_tiles, dtype=jnp.int32)
    name_row = (b // per_shard * rows + row_index) * per_shard + b % per_shard
    names = (name_row[:, None] * side + jnp.arange(win_tiles, dtype=jnp.int32)).reshape(-1)
    order = jnp.arange(slots, dtype=jnp.int32)
    slot_table = slots - jnp.max(
        jnp.where(names[:, None] == tile_list[None, :], slots - order, 0), axis=1
    )
    padded = nodes + 4 * LANES
    cfg = (cols, rows, lines, per_shard, tile, slots, nodes, layers, rhs, levels)
    smem = pl.BlockSpec(memory_space=pltpu.SMEM)
    vmem = pl.BlockSpec(memory_space=pltpu.VMEM)
    block = (per_shard, rhs, tile)
    dma = pltpu.SemaphoreType.DMA
    out = jax.ShapeDtypeStruct((rhs, shard), F32)
    return pl.pallas_call(
        functools.partial(kernel, cfg),
        out_shape=(out, out),
        in_specs=[smem] * 5 + [vmem] * 4 + [pl.BlockSpec(memory_space=pl.ANY)],
        out_specs=(vmem, vmem),
        scratch_shapes=[
            pltpu.VMEM((slots, tile, tile), BF16),
            pltpu.VMEM((ITERS,) + block, BF16),
            pltpu.VMEM((ITERS, cols) + block, BF16),
            pltpu.VMEM((ITERS, rows) + block, BF16),
            pltpu.VMEM((ITERS, lines, rhs, LANES), BF16),
            pltpu.VMEM((ITERS, lines, rhs, LANES), BF16),
            pltpu.VMEM((2, lines, layers, LANES), jnp.int32),
            pltpu.VMEM((2, lines, layers, LANES), F32),
            pltpu.VMEM((slots + 1, rhs, tile), F32),
            pltpu.VMEM((ITERS, rows) + block, BF16),
            pltpu.VMEM((ITERS, rows) + block, BF16),
            pltpu.VMEM((ITERS, cols) + block, BF16),
            pltpu.VMEM((ITERS, cols) + block, BF16),
            pltpu.VMEM((layers, padded), F32),
            pltpu.VMEM((layers, padded), F32),
            pltpu.VMEM((5, layers, SUB, padded), F32),
            pltpu.VMEM((2, layers, rhs, padded), F32),
            pltpu.VMEM((rhs, padded), F32),
            dma((slots,)),
            dma((ITERS, cols)),
            dma((ITERS, cols)),
            dma((ITERS, rows)),
            dma((ITERS, rows)),
            dma((ITERS, 2, lines)),
            dma((ITERS, 2, lines)),
            dma((2, 2)),
            dma((2, 2)),
            dma((ITERS, rows)),
            dma((ITERS, rows)),
            dma((ITERS, cols)),
            dma((ITERS, cols)),
            pltpu.VMEM((cols,) + block, BF16),
            pltpu.VMEM((rows,) + block, BF16),
            pltpu.VMEM((lines, rhs, LANES), BF16),
        ],
        compiler_params=pltpu.CompilerParams(
            collective_id=0, has_side_effects=True, vmem_limit_bytes=60 * 1024 * 1024
        ),
        name="coupled",
    )(
        band_tile,
        col_tile,
        slot_table,
        surf_map,
        coef_table,
        trace_start,
        surface_load,
        coef_index,
        vol_source,
        panel_tiles,
    )


def solution(mesh):
    return jax.shard_map(
        local,
        mesh=mesh,
        in_specs=(
            P(None, ("col", "row")),
            P(None, ("col", "row")),
            P(("col", "row"), None, None),
            P(("col", "row")),
            P(),
            P(None, None, "row"),
            P(),
            P(None, None, "row"),
        ),
        out_specs=(P(None, ("col", "row")), P(None, ("col", "row"))),
        check_vma=False,
    )
```

```python
import functools

import jax
import jax.numpy as jnp
from jax import lax
from jax.experimental import pallas as pl
from jax.experimental.pallas import tpu as pltpu
from jax.sharding import PartitionSpec as P

ITERS = 2
SWEEPS = 4

COUPLING_STEP = 0.3
JACOBI_WEIGHT = 0.8
CELL_MASS = 0.05

LANES = 128
SUB = 8
F32 = jnp.float32
BF16 = jnp.bfloat16


def kernel(
    cfg,
    row_tile_ref,
    col_tile_ref,
    slot_ref,
    surf_ref,
    table_ref,
    start_ref,
    load_ref,
    index_ref,
    source_ref,
    panel_hbm,
    traces_ref,
    response_ref,
    panel,
    own,
    band,
    window,
    edge_left,
    edge_right,
    halo_index,
    halo_source,
    product,
    window_part,
    window_recv,
    row_part,
    row_recv,
    coef_ext,
    source_ext,
    weights,
    state,
    top,
    panel_sem,
    band_send,
    band_recv,
    win_send,
    win_recv,
    edge_send,
    edge_recv,
    halo_send,
    halo_recv,
    part_send,
    part_recv,
    row_send,
    row_rsem,
    band_now,
    window_now,
    edge_now,
):
    cols, rows, lines, per_shard, tile, slots, nodes, layers, rhs, levels = cfg
    dense = cols - lines
    group = cols // lines
    shard = per_shard * tile
    win_tiles = rows * per_shard
    c = lax.axis_index("col")
    r = lax.axis_index("row")
    vol = jnp.maximum(c - dense, 0)
    row_up = jnp.minimum(r + 1, rows - 1)
    row_down = jnp.maximum(r - 1, 0)
    is_volume = c >= dense
    is_dense = c < dense
    first_of_tile = (lax.rem(c, group) == 0) & (r > 0)
    last_of_tile = (lax.rem(c, group) == group - 1) & (r < rows - 1)
    has_left = r > 0
    has_right = r < rows - 1

    def copy(src, dst, send, recv, to_col, to_row):
        return pltpu.make_async_remote_copy(
            src_ref=src,
            dst_ref=dst,
            send_sem=send,
            recv_sem=recv,
            device_id=(to_col, to_row),
            device_id_type=pl.DeviceIdType.MESH,
        )

    def col_peer(k):
        return lax.rem(c + k, cols)

    def row_peer(k):
        return lax.rem(r + k, rows)

    def panel_copy(s):
        return pltpu.make_async_copy(panel_hbm.at[s], panel.at[s], panel_sem.at[s])

    @pl.when(is_dense)
    def _():
        def start(s, _):
            panel_copy(s).start()
            return 0

        lax.fori_loop(0, slots, start, 0)

    barrier = pltpu.get_barrier_semaphore()

    def greet(to_col, to_row):
        pl.semaphore_signal(
            barrier, inc=1, device_id=(to_col, to_row), device_id_type=pl.DeviceIdType.MESH
        )

    for k in range(1, cols):
        greet(col_peer(k), r)
    for k in range(1, rows):
        greet(c, row_peer(k))

    @pl.when(last_of_tile)
    def _():
        for v in range(lines):
            greet(dense + v, row_up)

    @pl.when(first_of_tile)
    def _():
        for v in range(lines):
            greet(dense + v, row_down)

    @pl.when(is_volume & has_left)
    def _():
        for q in range(lines):
            greet(q * group + group - 1, row_down)

    @pl.when(is_volume & has_right)
    def _():
        for q in range(lines):
            greet(q * group, row_up)

    def count(flag):
        return jnp.where(flag, lines, 0)

    expected = (
        cols
        - 1
        + rows
        - 1
        + count(last_of_tile)
        + count(first_of_tile)
        + count(is_volume & has_left)
        + count(is_volume & has_right)
    )
    traces_ref[...] = start_ref[...]
    product[slots] = jnp.zeros((rhs, tile), F32)
    pl.semaphore_wait(barrier, expected)

    def halo_copy(kind, side, arrival=False):
        ref = (index_ref, source_ref)[kind]
        dst = (halo_index, halo_source)[kind]
        at = nodes - LANES if side == 0 else 0
        to = row_up if (side == 0) != arrival else row_down
        return copy(
            ref.at[:, :, pl.ds(at, LANES)],
            dst.at[side],
            halo_send.at[kind, side],
            halo_recv.at[kind, side],
            c,
            to,
        )

    sides = ((0, has_right, has_left), (1, has_left, has_right))
    for side, sends, _ in sides:

        @pl.when(is_volume & sends)
        def _():
            for kind in range(2):
                halo_copy(kind, side).start()

    def band_copy(it, k):
        to = col_peer(k)
        return copy(own.at[it], band.at[it, c], band_send.at[it, k], band_recv.at[it, c], to, r)

    def band_arrival(it, src):
        return copy(own.at[it], band.at[it, src], band_send.at[it, 0], band_recv.at[it, src], src, r)

    def edge_copy(it, side, v):
        q = lax.div(c, group)
        if side == 0:
            src = own.at[it, per_shard - 1, :, pl.ds(tile - LANES, LANES)]
            dst, to = edge_left, row_up
        else:
            src = own.at[it, 0, :, pl.ds(0, LANES)]
            dst, to = edge_right, row_down
        return copy(
            src,
            dst.at[it, q],
            edge_send.at[it, side, v],
            edge_recv.at[it, side, q],
            dense + v,
            to,
        )

    def edge_arrival(it, side, q):
        dst = (edge_left, edge_right)[side]
        src = own.at[it, 0, :, pl.ds(0, LANES)]
        if side == 0:
            from_col, from_row = q * group + group - 1, row_down
        else:
            from_col, from_row = q * group, row_up
        return copy(
            src,
            dst.at[it, q],
            edge_send.at[it, side, 0],
            edge_recv.at[it, side, q],
            from_col,
            from_row,
        )

    def window_copy(it, k):
        to = row_peer(k)
        return copy(band.at[it, 0], window.at[it, r], win_send.at[it, k], win_recv.at[it, r], c, to)

    def window_arrival(it, k):
        src = row_peer(k)
        return copy(
            band.at[it, 0], window.at[it, src], win_send.at[it, k], win_recv.at[it, src], c, src
        )

    def part_copy(it, k):
        to = row_peer(k)
        return copy(
            window_part.at[it, to],
            window_recv.at[it, r],
            part_send.at[it, k],
            part_recv.at[it, r],
            c,
            to,
        )

    def part_arrival(it, k):
        src = row_peer(k)
        return copy(
            window_part.at[it, src],
            window_recv.at[it, src],
            part_send.at[it, k],
            part_recv.at[it, src],
            c,
            src,
        )

    def row_copy(it, to):
        return copy(
            row_part.at[it, to], row_recv.at[it, c], row_send.at[it, to], row_rsem.at[it, c], to, r
        )

    def row_arrival(it, src):
        return copy(
            row_part.at[it, src],
            row_recv.at[it, src],
            row_send.at[it, src],
            row_rsem.at[it, src],
            src,
            r,
        )

    def prepare_volume():
        line = lax.div(surf_ref[r * lines + vol], rows)
        padded = nodes + 4 * LANES
        for side, _, receives in sides:

            @pl.when(receives)
            def _():
                for kind in range(2):
                    halo_copy(kind, side, True).wait_recv()

            @pl.when(jnp.logical_not(receives))
            def _():
                halo_index[side] = jnp.zeros((lines, layers, LANES), jnp.int32)
                halo_source[side] = jnp.zeros((lines, layers, LANES), F32)

        def lookup(indices):
            values = jnp.zeros(indices.shape, F32)
            for level in range(levels):
                values = jnp.where(indices == level, table_ref[level], values)
            return values

        zeros = jnp.zeros((layers, LANES), F32)
        left_on = jnp.where(has_left, 1.0, 0.0)
        right_on = jnp.where(has_right, 1.0, 0.0)
        right_at = 2 * LANES + nodes
        coef_ext[:, 0:LANES] = zeros
        coef_ext[:, LANES : 2 * LANES] = lookup(halo_index[0, line]) * left_on
        coef_ext[:, 2 * LANES : right_at] = lookup(index_ref[line])
        coef_ext[:, right_at : right_at + LANES] = lookup(halo_index[1, line]) * right_on
        coef_ext[:, right_at + LANES :] = zeros
        source_ext[:, 0:LANES] = zeros
        source_ext[:, LANES : 2 * LANES] = halo_source[0, line]
        source_ext[:, 2 * LANES : right_at] = source_ref[line]
        source_ext[:, right_at : right_at + LANES] = halo_source[1, line]
        source_ext[:, right_at + LANES :] = zeros
        lane = lax.broadcasted_iota(jnp.int32, (1, padded), 1)
        low = jnp.where(has_left, LANES, 2 * LANES)
        high = jnp.where(has_right, right_at + LANES, right_at)
        inside = (lane >= low) & (lane < high)
        for layer in range(layers):
            k = coef_ext[layer : layer + 1, :]
            left = 0.5 * (k + pltpu.roll(k, 1, 1))
            right = 0.5 * (k + pltpu.roll(k, padded - 1, 1))
            up = 0.5 * (k + coef_ext[layer - 1 : layer, :]) if layer else k
            diagonal = left + right + up + CELL_MASS
            parts = [left, right, up]
            if layer < layers - 1:
                down = 0.5 * (k + coef_ext[layer + 1 : layer + 2, :])
                diagonal = diagonal + down
                parts.append(down)
            else:
                parts.append(None)
            parts.append(source_ext[layer : layer + 1, :])
            scale = jnp.where(inside, JACOBI_WEIGHT / diagonal, 0.0)
            for kind, part in enumerate(parts):
                if part is not None:
                    weights[kind, layer] = jnp.broadcast_to(part * scale, (SUB, padded))
        top[:, 0:LANES] = jnp.zeros((rhs, LANES), F32)
        top[:, right_at + LANES :] = jnp.zeros((rhs, LANES), F32)
        for layer in range(layers):
            state[0, layer] = jnp.zeros((rhs, padded), F32)
            state[1, layer, :, 0:LANES] = jnp.zeros((rhs, LANES), F32)
            state[1, layer, :, right_at + LANES :] = jnp.zeros((rhs, LANES), F32)

    def relax(now, at, width):
        span = width + 2 * LANES
        begin = pl.multiple_of(at - LANES, LANES)
        at = pl.multiple_of(at, LANES)
        for layer in range(layers):
            factors = [
                None if kind == 3 and layer == layers - 1 else weights[kind, layer, :, pl.ds(at, width)]
                for kind in range(5)
            ]
            for g in range(rhs // SUB):
                lines_at = pl.ds(g * SUB, SUB)
                around = state[now, layer, lines_at, pl.ds(begin, span)]
                centre = around[:, LANES : LANES + width]
                before = pltpu.roll(around, 1, 1)[:, LANES : LANES + width]
                after = pltpu.roll(around, span - 1, 1)[:, LANES : LANES + width]
                if layer:
                    above = state[now, layer - 1, lines_at, pl.ds(at, width)]
                else:
                    above = top[lines_at, pl.ds(at, width)]
                value = (1.0 - JACOBI_WEIGHT) * centre + factors[4]
                value = value + factors[0] * before + factors[1] * after + factors[2] * above
                if layer < layers - 1:
                    value = value + factors[3] * state[now, layer + 1, lines_at, pl.ds(at, width)]
                state[1 - now, layer, lines_at, pl.ds(at, width)] = value

    def volume(it):
        q = vol
        right_at = 2 * LANES + nodes
        for m in range(group):
            src = q * group + m

            @pl.when(src != c)
            def _():
                band_arrival(it, src).wait_recv()

            for p in range(per_shard):
                at = 2 * LANES + m * shard + p * tile
                top[:, at : at + tile] = band[it, src, p].astype(F32)
        line = lax.div(surf_ref[r * lines + q], rows)
        for side, _, receives in sides:
            dst = (edge_left, edge_right)[side]
            at = LANES if side == 0 else right_at
            base = row_down if side == 0 else row_up
            place = 0
            for z in range(lines):
                place = jnp.where(surf_ref[base * lines + z] == line * rows + base, z, place)

            @pl.when(receives)
            def _():
                for z in range(lines):
                    edge_arrival(it, side, z).wait_recv()
                for z in range(lines):
                    edge_now[z] = dst[it, z]
                top[:, at : at + LANES] = edge_now[place].astype(F32)

            @pl.when(jnp.logical_not(receives))
            def _():
                top[:, at : at + LANES] = jnp.zeros((rhs, LANES), F32)

        width = 2 * tile

        def sweep(now):
            relax(now, LANES, LANES)
            relax(now, right_at, LANES)

            def chunk(j, _):
                relax(now, 2 * LANES + j * width, width)
                return 0

            lax.fori_loop(0, nodes // width, chunk, 0)

        for i in range(SWEEPS):
            sweep(i % 2)
        done = SWEEPS % 2
        for m in range(group):
            to = q * group + m
            for p in range(per_shard):
                at = 2 * LANES + m * shard + p * tile
                k = index_coef(at)
                flux = k * (top[:, at : at + tile] - state[done, 0, :, at : at + tile])
                row_part[it, to, p] = flux.astype(BF16)

            @pl.when(to != c)
            def _():
                row_copy(it, to).start()

    def index_coef(at):
        return coef_ext[0:1, at : at + tile]

    def total_of(tiles_of):
        value = product[tiles_of[0]]
        for t in tiles_of[1:]:
            value = value + product[t]
        return value

    def dense_part(it):
        @pl.when(c != 0)
        def _():
            band_arrival(it, 0).wait_recv()

        for k in range(1, rows):
            window_copy(it, k).start()
        window[it, r] = band[it, 0]
        for src in range(1, cols):

            @pl.when(c != src)
            def _():
                band_arrival(it, src).wait_recv()

        for src in range(cols):
            band_now[src] = band[it, src]

        def into_cols(s, _):
            @pl.when(it == 0)
            def _():
                panel_copy(s).wait()

            row_tile = row_tile_ref[s]
            traces = band_now[lax.div(row_tile, per_shard), lax.rem(row_tile, per_shard)]
            product[s] = jnp.dot(traces, panel[s], preferred_element_type=F32)
            return 0

        lax.fori_loop(0, slots, into_cols, 0)
        band_tiles = cols * per_shard

        def sum_window(j, _):
            value = total_of([slot_ref[b * win_tiles + j] for b in range(band_tiles)])
            window_part[it, lax.div(j, per_shard), lax.rem(j, per_shard)] = value.astype(BF16)
            return 0

        lax.fori_loop(0, win_tiles, sum_window, 0)
        for k in range(1, rows):
            part_copy(it, k).start()
        for k in range(1, rows):
            window_arrival(it, k).wait_recv()

        for src in range(rows):
            window_now[src] = window[it, src]

        def into_rows(s, _):
            col_tile = col_tile_ref[s]
            traces = window_now[lax.div(col_tile, per_shard), lax.rem(col_tile, per_shard)]
            product[s] = lax.dot_general(
                traces, panel[s], (((1,), (1,)), ((), ())), preferred_element_type=F32
            )
            return 0

        lax.fori_loop(0, slots, into_rows, 0)

        def sum_rows(b, _):
            value = total_of([slot_ref[b * win_tiles + j] for j in range(win_tiles)])
            row_part[it, lax.div(b, per_shard), lax.rem(b, per_shard)] = value.astype(BF16)
            return 0

        lax.fori_loop(per_shard, band_tiles, sum_rows, 0)
        for to in range(1, cols):

            @pl.when(c != to)
            def _():
                row_copy(it, to).start()

        for k in range(1, rows):
            part_arrival(it, k).wait_recv()
        for p in range(per_shard):
            value = total_of([slot_ref[p * win_tiles + j] for j in range(win_tiles)])
            value = value + window_part[it, r, p].astype(F32)
            for k in range(1, rows):
                value = value + window_recv[it, row_peer(k), p].astype(F32)
            row_part[it, 0, p] = value.astype(BF16)

        @pl.when(c != 0)
        def _():
            row_copy(it, 0).start()

    def iteration(it, _):
        for p in range(per_shard):
            rounded = traces_ref[:, p * tile : (p + 1) * tile].astype(BF16)
            own[it, p] = rounded
            band[it, c, p] = rounded
        for k in range(1, cols):
            band_copy(it, k).start()
        for side, flag in ((0, last_of_tile), (1, first_of_tile)):

            @pl.when(flag)
            def _():
                for v in range(lines):
                    edge_copy(it, side, v).start()

        @pl.when(is_volume)
        def _():
            @pl.when(it == 0)
            def _():
                prepare_volume()

            volume(it)
            for k in range(cols):

                @pl.when((k != c) & (k // group != c - dense))
                def _():
                    band_arrival(it, k).wait_recv()

        @pl.when(is_dense)
        def _():
            dense_part(it)

        owner = dense + lax.div(c, group)
        for src in range(cols):

            @pl.when((src != c) & ((src < dense) | (src == owner)))
            def _():
                row_arrival(it, src).wait_recv()

        def own_part(p):
            return row_part[it, c, p].astype(F32)

        for p in range(per_shard):
            at = slice(p * tile, (p + 1) * tile)
            response_ref[:, at] = jnp.zeros((rhs, tile), F32)
            for src in range(dense):

                @pl.when(src != c)
                def _():
                    response_ref[:, at] += row_recv[it, src, p].astype(F32)

            @pl.when(owner != c)
            def _():
                response_ref[:, at] += row_recv[it, owner, p].astype(F32)

            @pl.when(is_dense | (owner == c))
            def _():
                response_ref[:, at] += own_part(p)

            t = traces_ref[:, at]
            traces_ref[:, at] = t + COUPLING_STEP * (load_ref[:, at] - t - response_ref[:, at])
        return 0

    lax.fori_loop(0, ITERS, iteration, 0)

    def drain(it, _):
        for k in range(1, cols):
            band_copy(it, k).wait_send()
        for side, flag in ((0, last_of_tile), (1, first_of_tile)):

            @pl.when(flag)
            def _():
                for v in range(lines):
                    edge_copy(it, side, v).wait_send()

        @pl.when(is_dense)
        def _():
            for k in range(1, rows):
                window_copy(it, k).wait_send()
                part_copy(it, k).wait_send()
            for to in range(cols):

                @pl.when(c != to)
                def _():
                    row_copy(it, to).wait_send()

        @pl.when(is_volume)
        def _():
            for m in range(group):
                to = vol * group + m

                @pl.when(to != c)
                def _():
                    row_copy(it, to).wait_send()

        return 0

    lax.fori_loop(0, ITERS, drain, 0)
    for side, sends, _ in sides:

        @pl.when(is_volume & sends)
        def _():
            for kind in range(2):
                halo_copy(kind, side).wait_send()


def local(
    trace_start, surface_load, panel_tiles, tile_list, surf_map, coef_index, coef_table, vol_source
):
    cols = lax.axis_size("col")
    rows = lax.axis_size("row")
    row_index = lax.axis_index("row")
    lines, layers, nodes = coef_index.shape
    slots, tile, _ = panel_tiles.shape
    rhs, shard = trace_start.shape
    per_shard = shard // tile
    levels = coef_table.shape[0]
    side = cols * rows * per_shard
    band_tiles = cols * per_shard
    win_tiles = rows * per_shard
    safe = jnp.maximum(tile_list, 0)
    row_tile = safe // side
    col_tile = safe % side
    band_tile = row_tile // per_shard // rows * per_shard + row_tile % per_shard
    b = jnp.arange(band_tiles, dtype=jnp.int32)
    name_row = (b // per_shard * rows + row_index) * per_shard + b % per_shard
    names = (name_row[:, None] * side + jnp.arange(win_tiles, dtype=jnp.int32)).reshape(-1)
    order = jnp.arange(slots, dtype=jnp.int32)
    slot_table = slots - jnp.max(
        jnp.where(names[:, None] == tile_list[None, :], slots - order, 0), axis=1
    )
    padded = nodes + 4 * LANES
    cfg = (cols, rows, lines, per_shard, tile, slots, nodes, layers, rhs, levels)
    smem = pl.BlockSpec(memory_space=pltpu.SMEM)
    vmem = pl.BlockSpec(memory_space=pltpu.VMEM)
    block = (per_shard, rhs, tile)
    dma = pltpu.SemaphoreType.DMA
    out = jax.ShapeDtypeStruct((rhs, shard), F32)
    return pl.pallas_call(
        functools.partial(kernel, cfg),
        out_shape=(out, out),
        in_specs=[smem] * 5 + [vmem] * 4 + [pl.BlockSpec(memory_space=pl.ANY)],
        out_specs=(vmem, vmem),
        scratch_shapes=[
            pltpu.VMEM((slots, tile, tile), BF16),
            pltpu.VMEM((ITERS,) + block, BF16),
            pltpu.VMEM((ITERS, cols) + block, BF16),
            pltpu.VMEM((ITERS, rows) + block, BF16),
            pltpu.VMEM((ITERS, lines, rhs, LANES), BF16),
            pltpu.VMEM((ITERS, lines, rhs, LANES), BF16),
            pltpu.VMEM((2, lines, layers, LANES), jnp.int32),
            pltpu.VMEM((2, lines, layers, LANES), F32),
            pltpu.VMEM((slots + 1, rhs, tile), F32),
            pltpu.VMEM((ITERS, rows) + block, BF16),
            pltpu.VMEM((ITERS, rows) + block, BF16),
            pltpu.VMEM((ITERS, cols) + block, BF16),
            pltpu.VMEM((ITERS, cols) + block, BF16),
            pltpu.VMEM((layers, padded), F32),
            pltpu.VMEM((layers, padded), F32),
            pltpu.VMEM((5, layers, SUB, padded), F32),
            pltpu.VMEM((2, layers, rhs, padded), F32),
            pltpu.VMEM((rhs, padded), F32),
            dma((slots,)),
            dma((ITERS, cols)),
            dma((ITERS, cols)),
            dma((ITERS, rows)),
            dma((ITERS, rows)),
            dma((ITERS, 2, lines)),
            dma((ITERS, 2, lines)),
            dma((2, 2)),
            dma((2, 2)),
            dma((ITERS, rows)),
            dma((ITERS, rows)),
            dma((ITERS, cols)),
            dma((ITERS, cols)),
            pltpu.VMEM((cols,) + block, BF16),
            pltpu.VMEM((rows,) + block, BF16),
            pltpu.VMEM((lines, rhs, LANES), BF16),
        ],
        compiler_params=pltpu.CompilerParams(
            collective_id=0, has_side_effects=True, vmem_limit_bytes=60 * 1024 * 1024
        ),
        name="coupled",
    )(
        band_tile,
        col_tile,
        slot_table,
        surf_map,
        coef_table,
        trace_start,
        surface_load,
        coef_index,
        vol_source,
        panel_tiles,
    )


def solution(mesh):
    return jax.shard_map(
        local,
        mesh=mesh,
        in_specs=(
            P(None, ("col", "row")),
            P(None, ("col", "row")),
            P(("col", "row"), None, None),
            P(("col", "row")),
            P(),
            P(None, None, "row"),
            P(),
            P(None, None, "row"),
        ),
        out_specs=(P(None, ("col", "row")), P(None, ("col", "row"))),
        check_vma=False,
    )
```
